256 devices in a mesh: pencil: 64 (over y, x_lo, z), angle: 4 (over x_hi, core).
Axes of the slice: x: 4 (x_hi: 2, x_lo: 2; x = x_hi * 2 + x_lo), y: 4, z: 8, core: 2. Of those that a mesh axis runs over, the one named last changes fastest.
Arguments:
- tomo_real: bfloat16 [512, 512, 128], P(None, 'pencil'), may hold values from -6 to 6
- tomo_imag: bfloat16 [512, 512, 128], P(None, 'pencil'), may hold values from -6 to 6
- template_real: bfloat16 [8, 512, 512, 128], P('angle', None, 'pencil'), may hold values from -6 to 6
- template_imag: bfloat16 [8, 512, 512, 128], P('angle', None, 'pencil'), may hold values from -6 to 6
- wedge_flags: int32 [512, 512, 128], P(None, 'pencil'), may hold values 0 or 1
- local_sigma: float32 [512, 512, 128], P('pencil'), may hold values from 0.5 to 2
Outputs:
- best_score: float32 [512, 512, 128], P('pencil', 'angle')
- runner_up: float32 [512, 512, 128], P('pencil', 'angle')
The draws below stay inside these ranges and needn't reach their ends.
All inputs are finite; a program needn't handle non-finite values. No bound on the sum of `wedge_flags` on one device may be relied on, other than what follows from the above.
Results may differ from the reference program's by a relative error of at most 0.0064.
Values may be sent and summed in bfloat16 or wider, within the bound.
No kernel may reach another device: no remote copies, remote signals or barrier semaphores. Data moves between devices by JAX's collectives and lax.ppermute only.
A program may use at most 128 MiB of HBM per device.

```python
import math
import jax
import jax.numpy as jnp
from jax import lax

X = 512
Y = 512
Z = 128
ANGLES = 8


def set_ends(entries, own_key, least, high):
    extent = entries.shape
    spot = [jax.random.randint(jax.random.fold_in(own_key, axis), (), 0, extent[axis]) for axis in range(len(extent))]
    entries = entries.at[tuple(spot)].set(least)
    longest = extent.index(max(extent))
    spot[longest] = (spot[longest] + 1) % extent[longest]
    return entries.at[tuple(spot)].set(high)


def shard_levels(own_key, dims, cuts, smallest, high):
    def one(position, blocks):
        draws = jax.random.uniform(jax.random.fold_in(jax.random.fold_in(own_key, 6), position), (blocks,), jnp.float32, smallest / len(cuts), high / len(cuts))
        return jnp.repeat(jnp.exp(draws), dims[position] // blocks).reshape((-1,) + (1,) * (len(dims) - position - 1))

    gain = one(*cuts[0])
    for cut in cuts[1:]:
        gain = gain * one(*cut)
    return gain


def gaussian(own_key, extent, scale, limit, shards=(), held_as=jnp.bfloat16):
    result = scale * jax.random.normal(own_key, extent, jnp.float32)
    if shards:
        result = result * shard_levels(own_key, extent, shards, -0.22, 0.18)
    return jnp.clip(result, -limit, limit).astype(held_as)


def setup_inputs(seed: int = 0) -> dict:
    splits = jax.random.split(jax.random.key(seed), 7)
    tomo_real = gaussian(splits[0], (X, Y, Z), 1.0, 6.0, ((1, 64),))
    tomo_imag = gaussian(splits[1], (X, Y, Z), 1.0, 6.0, ((1, 64),))
    template_real = gaussian(splits[2], (ANGLES, X, Y, Z), 1.0, 6.0, ((0, 4), (2, 64)))
    template_imag = gaussian(splits[3], (ANGLES, X, Y, Z), 1.0, 6.0, ((0, 4), (2, 64)))
    wedge_flags = set_ends((jax.random.randint(splits[4], (X, Y, Z), 0, 2) < 1).astype(jnp.int32), jax.random.fold_in(splits[4], 1), 0, 1)
    local_sigma = jnp.clip(jnp.exp(math.log(2.0) - 1.3862944 * jax.random.uniform(splits[5], (X, Y, Z), jnp.float32) ** shard_levels(splits[5], (X, Y, Z), ((0, 64),), -0.2, 0.2)), 0.5, 2.0)
    return {"tomo_real": tomo_real, "tomo_imag": tomo_imag, "template_real": template_real, "template_imag": template_imag, "wedge_flags": wedge_flags, "local_sigma": local_sigma}


def make_tables(length):
    positions = jnp.arange(length, dtype=jnp.int32)
    products = positions[:, None] * positions[None, :] % length
    phases = products.astype(jnp.float32) * (2.0 * math.pi / length)
    return (jnp.cos(phases).astype(jnp.bfloat16), jnp.sin(phases).astype(jnp.bfloat16))

def reference(tomo_real, tomo_imag, template_real, template_imag, wedge_flags, local_sigma):
    cos_z, sin_z = make_tables(Z)
    cos_x, sin_x = make_tables(X)
    cos_y, sin_y = make_tables(Y)
    flags = wedge_flags.astype(jnp.float32)
    spec_real = tomo_real.astype(jnp.float32)
    spec_imag = tomo_imag.astype(jnp.float32)
    norm_scale = 1.0 / math.sqrt(X * Y * Z)

    def one_angle(carry, pieces):
        best_score, runner_up = carry
        temp_real = pieces[0].astype(jnp.float32)
        temp_imag = pieces[1].astype(jnp.float32)
        prod_real = (flags * (spec_real * temp_real + spec_imag * temp_imag)).astype(jnp.bfloat16).reshape(X * Y, Z)
        prod_imag = (flags * (spec_imag * temp_real - spec_real * temp_imag)).astype(jnp.bfloat16).reshape(X * Y, Z)
        first_real = (jnp.dot(prod_real, cos_z, preferred_element_type=jnp.float32) - jnp.dot(prod_imag, sin_z, preferred_element_type=jnp.float32)).astype(jnp.bfloat16).reshape(X, Y * Z)
        first_imag = (jnp.dot(prod_real, sin_z, preferred_element_type=jnp.float32) + jnp.dot(prod_imag, cos_z, preferred_element_type=jnp.float32)).astype(jnp.bfloat16).reshape(X, Y * Z)
        second_real = (jnp.dot(cos_x, first_real, preferred_element_type=jnp.float32) - jnp.dot(sin_x, first_imag, preferred_element_type=jnp.float32)).astype(jnp.bfloat16)
        second_imag = (jnp.dot(sin_x, first_real, preferred_element_type=jnp.float32) + jnp.dot(cos_x, first_imag, preferred_element_type=jnp.float32)).astype(jnp.bfloat16)
        moved_real = jnp.transpose(second_real.reshape(X, Y, Z), (1, 0, 2)).reshape(Y, X * Z)
        moved_imag = jnp.transpose(second_imag.reshape(X, Y, Z), (1, 0, 2)).reshape(Y, X * Z)
        correlation = jnp.dot(cos_y, moved_real, preferred_element_type=jnp.float32) - jnp.dot(sin_y, moved_imag, preferred_element_type=jnp.float32)
        correlation = jnp.transpose(correlation.reshape(Y, X, Z), (1, 0, 2)) * norm_scale
        scores = correlation / local_sigma
        new_runner = jnp.maximum(runner_up, jnp.minimum(best_score, scores))
        new_best = jnp.maximum(best_score, scores)
        return ((new_best, new_runner), None)
    start = jnp.full((X, Y, Z), -1e+30, dtype=jnp.float32)
    (best_score, runner_up), unused = lax.scan(one_angle, (start, start), (template_real, template_imag))
    return (best_score, runner_up)
```

```python
import math

import jax
import jax.numpy as jnp
import numpy as np
from jax import lax
from jax.experimental import pallas as pl
from jax.experimental.pallas import tpu as pltpu
from jax.sharding import PartitionSpec as P

CHUNKS = (4, 4)
CORE = ((0, 1), (1, 0), (2, 3), (3, 2))
FAR = ((0, 2), (1, 3), (2, 0), (3, 1))


def phases(length):
    k = np.arange(length, dtype=np.int64)
    angle = (k[:, None] * k[None, :] % length) * (2.0 * math.pi / length)
    return np.cos(angle), np.sin(angle)


def z_table(size_z):
    cos, sin = phases(size_z)
    return np.block([[cos, sin], [-sin, cos]]).astype(jnp.bfloat16)


def x_table(size_x, groups, first, count):
    cos, sin = phases(size_x)
    each = size_x // groups
    rows = (np.arange(groups)[:, None] * each + np.arange(first, first + count)[None, :]).reshape(-1)
    return np.concatenate([cos[rows], sin[rows]], 0).astype(jnp.bfloat16)


def y_table(size_y, groups):
    cos, sin = phases(size_y)
    both = np.stack([cos.reshape(size_y, groups, -1), -sin.reshape(size_y, groups, -1)], 2)
    return both.reshape(size_y, -1).astype(jnp.bfloat16)


def along_z(tr, ti, ar, ai, flags, table, out, tmp):
    block, rows, size_z = tr.shape
    flag = flags[...].astype(jnp.float32)
    fr = tr[...].astype(jnp.float32) * flag
    fi = ti[...].astype(jnp.float32) * flag
    for a in range(ar.shape[0]):
        br = ar[a].astype(jnp.float32)
        bi = ai[a].astype(jnp.float32)
        pr = (fr * br + fi * bi).astype(jnp.bfloat16).reshape(block * rows, size_z)
        pi = (fi * br - fr * bi).astype(jnp.bfloat16).reshape(block * rows, size_z)
        both = jnp.concatenate([pr, pi], 1)
        sums = jnp.dot(both, table[...], preferred_element_type=jnp.float32)
        tmp[2 * a] = sums[:, :size_z]
        tmp[2 * a + 1] = sums[:, size_z:]
        for k in range(rows):
            half = [tmp[2 * a + h, pl.ds(k, block, stride=rows), :] for h in range(2)]
            out[a, k] = jnp.concatenate(half, 1).astype(jnp.bfloat16)


def along_x(q, table, out, tmp):
    rows, _, width = q.shape[1:]
    size_z = width // 2
    half = table.shape[0] // 2

    def one(k, carry):
        both = jnp.dot(table[...], q[0, k], preferred_element_type=jnp.float32)
        tmp[pl.ds(k, half, stride=2 * rows), :] = both[:half, :size_z] - both[half:, size_z:]
        tmp[pl.ds(k + rows, half, stride=2 * rows), :] = both[half:, :size_z] + both[:half, size_z:]
        return carry

    lax.fori_loop(0, rows, one, 0)
    out[...] = tmp[...].astype(jnp.bfloat16).reshape(out.shape)


def along_y(who, got, sigma, table, keep, send, *, scale):
    groups, angles, count, pair, size_z = got.shape
    me = who[0]
    part = table.shape[0] // 4
    starts = [pl.multiple_of(jnp.bitwise_xor(me, r) * part, part) for r in range(4)]
    left = jnp.concatenate([table[pl.ds(s, part), :] for s in starts], 0)
    sums = []
    for a in range(angles):
        right = jnp.concatenate([got[:, a, i].reshape(groups * pair, size_z) for i in range(count)], 1)
        sums.append(jnp.dot(left, right, preferred_element_type=jnp.float32))
    for i in range(count):
        for r in range(4):
            here = (slice(r * part, (r + 1) * part), slice(i * size_z, (i + 1) * size_z))
            inverse = scale / sigma[i, pl.ds(starts[r], part), :]
            best = sums[0][here] * inverse
            runner = jnp.full_like(best, -1e30)
            for a in range(1, angles):
                score = sums[a][here] * inverse
                runner = jnp.maximum(runner, jnp.minimum(best, score))
                best = jnp.maximum(best, score)
            to = send if r % 2 else keep
            to[r // 2, 0, i] = best.astype(jnp.bfloat16)
            to[r // 2, 1, i] = runner.astype(jnp.bfloat16)


def top_two(first, later):
    best = jnp.maximum(first[0], later[0])
    return best, jnp.maximum(jnp.minimum(first[0], later[0]), jnp.maximum(first[1], later[1]))


def join_core(mine, other, keep, send):
    for slot, to in enumerate((keep, send)):
        best, runner = top_two((mine[slot, 0], mine[slot, 1]), (other[slot, 0], other[slot, 1]))
        to[0] = best
        to[1] = runner


def join_far(*refs):
    parts, (best_out, runner_out) = refs[:-2], refs[-2:]
    at = 0
    for mine, other in zip(parts[::2], parts[1::2]):
        best, runner = top_two((mine[0], mine[1]), (other[0], other[1]))
        best_out[at : at + mine.shape[1]] = best.astype(jnp.float32)
        runner_out[at : at + mine.shape[1]] = runner.astype(jnp.float32)
        at += mine.shape[1]


def cost(flops, moved):
    return pl.CostEstimate(flops=flops, bytes_accessed=moved, transcendentals=0)


def on_device(tomo_real, tomo_imag, template_real, template_imag, wedge_flags, local_sigma):
    size_x, rows, size_z = tomo_real.shape
    angles = template_real.shape[0]
    size_y = local_sigma.shape[1]
    groups = size_y // rows
    part = size_y // 4
    scale = 1.0 / math.sqrt(size_x * size_y * size_z)
    block = 64
    params = pltpu.CompilerParams(vmem_limit_bytes=48 * 1024 * 1024)

    spectrum = pl.pallas_call(
        along_z,
        grid=(size_x // block,),
        in_specs=[
            pl.BlockSpec((block, rows, size_z), lambda i: (i, 0, 0)),
            pl.BlockSpec((block, rows, size_z), lambda i: (i, 0, 0)),
            pl.BlockSpec((angles, block, rows, size_z), lambda i: (0, i, 0, 0)),
            pl.BlockSpec((angles, block, rows, size_z), lambda i: (0, i, 0, 0)),
            pl.BlockSpec((block, rows, size_z), lambda i: (i, 0, 0)),
            pl.BlockSpec((2 * size_z, 2 * size_z), lambda i: (0, 0)),
        ],
        out_specs=pl.BlockSpec((angles, rows, block, 2 * size_z), lambda i: (0, 0, i, 0)),
        out_shape=jax.ShapeDtypeStruct((angles, rows, size_x, 2 * size_z), jnp.bfloat16),
        scratch_shapes=[pltpu.VMEM((2 * angles, block * rows, size_z), jnp.float32)],
        compiler_params=params,
        cost_estimate=cost(8 * angles * size_x * rows * size_z * size_z, 12 * 2**20),
        name="along_z",
    )(tomo_real, tomo_imag, template_real, template_imag, wedge_flags, z_table(size_z))

    me = lax.axis_index("angle").astype(jnp.int32)[None]
    columns = y_table(size_y, groups)
    first = 0
    sent = []
    for count in CHUNKS:
        table = x_table(size_x, groups, first, count)
        sent.append(
            pl.pallas_call(
                along_x,
                grid=(angles,),
                in_specs=[
                    pl.BlockSpec((1, rows, size_x, 2 * size_z), lambda a: (a, 0, 0, 0)),
                    pl.BlockSpec(table.shape, lambda a: (0, 0)),
                ],
                out_specs=pl.BlockSpec((groups, 1, count, 2 * rows, size_z), lambda a: (0, a, 0, 0, 0)),
                out_shape=jax.ShapeDtypeStruct((groups, angles, count, 2 * rows, size_z), jnp.bfloat16),
                scratch_shapes=[pltpu.VMEM((groups * count * 2 * rows, size_z), jnp.float32)],
                compiler_params=params,
                cost_estimate=cost(8 * angles * size_x * groups * count * rows * size_z, 8 * 2**20),
                name="along_x",
            )(spectrum, table)
        )
        first += count

    joined = []
    first = 0
    for count, piece in zip(CHUNKS, sent):
        got = lax.all_to_all(piece, "pencil", split_axis=0, concat_axis=0, tiled=True)
        offset = first // 2
        out = jax.ShapeDtypeStruct((2, 2, count, part, size_z), jnp.bfloat16)
        keep, send = pl.pallas_call(
            lambda *refs: along_y(*refs, scale=scale),
            grid=(count // 2,),
            in_specs=[
                pl.BlockSpec(memory_space=pltpu.SMEM),
                pl.BlockSpec((groups, angles, 2, 2 * rows, size_z), lambda i: (0, 0, i, 0, 0)),
                pl.BlockSpec((2, size_y, size_z), lambda i, offset=offset: (i + offset, 0, 0)),
                pl.BlockSpec(columns.shape, lambda i: (0, 0)),
            ],
            out_specs=[pl.BlockSpec((2, 2, 2, part, size_z), lambda i: (0, 0, i, 0, 0))] * 2,
            out_shape=[out, out],
            compiler_params=params,
            cost_estimate=cost(4 * angles * count * size_y * size_y * size_z, 2 * 2**20 * count),
            name="along_y",
        )(me, got, local_sigma, columns)
        other = lax.ppermute(send, "angle", CORE)
        near = jax.ShapeDtypeStruct((2, count, part, size_z), jnp.bfloat16)
        keep, send = pl.pallas_call(
            join_core,
            out_shape=[near, near],
            compiler_params=params,
            cost_estimate=cost(2**20 * count, 2**19 * count),
            name="join_core",
        )(keep, other)
        joined += [keep, lax.ppermute(send, "angle", FAR)]
        first += count

    done = jax.ShapeDtypeStruct((local_sigma.shape[0], part, size_z), jnp.float32)
    return tuple(
        pl.pallas_call(
            join_far,
            out_shape=[done, done],
            compiler_params=params,
            cost_estimate=cost(2**20, 2**21),
            name="join_far",
        )(*joined)
    )


def solution(mesh):
    in_specs = (
        P(None, "pencil", None),
        P(None, "pencil", None),
        P("angle", None, "pencil", None),
        P("angle", None, "pencil", None),
        P(None, "pencil", None),
        P("pencil", None, None),
    )
    out_specs = (P("pencil", "angle", None), P("pencil", "angle", None))
    return jax.shard_map(
        on_device, mesh=mesh, in_specs=in_specs, out_specs=out_specs, check_vma=False
    )
```

```python
import math

import jax
import jax.numpy as jnp
import numpy as np
from jax import lax
from jax.experimental import pallas as pl
from jax.experimental.pallas import tpu as pltpu
from jax.sharding import PartitionSpec as P

CHUNKS = (6, 2)
CORE = ((0, 1), (1, 0), (2, 3), (3, 2))
FAR = ((0, 2), (1, 3), (2, 0), (3, 1))


def phases(length):
    k = np.arange(length, dtype=np.int64)
    angle = (k[:, None] * k[None, :] % length) * (2.0 * math.pi / length)
    return np.cos(angle), np.sin(angle)


def z_table(size_z):
    cos, sin = phases(size_z)
    return np.block([[cos, sin], [-sin, cos]]).astype(jnp.bfloat16)


def x_table(size_x, groups, first, count):
    cos, sin = phases(size_x)
    each = size_x // groups
    rows = (np.arange(groups)[:, None] * each + np.arange(first, first + count)[None, :]).reshape(-1)
    return np.concatenate([cos[rows], sin[rows]], 0).astype(jnp.bfloat16)


def y_table(size_y, groups):
    cos, sin = phases(size_y)
    both = np.stack([cos.reshape(size_y, groups, -1), -sin.reshape(size_y, groups, -1)], 2)
    return both.reshape(size_y, -1).astype(jnp.bfloat16)


def spin(q, table, tmp, put, unroll):
    rows, _, width = q.shape
    size_z = width // 2
    half = table.shape[0] // 2

    def one(k, carry):
        both = jnp.dot(table[...], q[k], preferred_element_type=jnp.float32)
        tmp[0, pl.ds(k, half, stride=rows), :] = both[:half, :size_z] - both[half:, size_z:]
        tmp[1, pl.ds(k, half, stride=rows), :] = both[half:, :size_z] + both[:half, size_z:]
        return carry

    lax.fori_loop(0, rows, one, 0, unroll=unroll)
    pair = [tmp[h].reshape(half, rows, size_z) for h in range(2)]
    put(jnp.concatenate(pair, 1).astype(jnp.bfloat16))


def front(tr, ti, ar, ai, flags, z_tab, x_tab, q_out, sent_out, *scratch):
    btr, bti, bar, bai, bfl, bz, bx, tmp, q, wide, sent, sems, more = scratch
    angles, size_x, rows, size_z = bar.shape
    blocks = sems.shape[0]
    block = size_x // blocks

    def copies(b):
        at = pl.ds(pl.multiple_of(b * block, block), block)
        pairs = [(tr.at[at], btr.at[at]), (ti.at[at], bti.at[at]), (flags.at[at], bfl.at[at])]
        pairs += [(ar.at[:, at], bar.at[:, at]), (ai.at[:, at], bai.at[:, at])]
        return [pltpu.make_async_copy(s, d, sems.at[b, j]) for j, (s, d) in enumerate(pairs)]

    def begin(b, carry):
        for c in copies(b):
            c.start()
        return carry

    tables = [
        pltpu.make_async_copy(z_tab, bz, more.at[0]),
        pltpu.make_async_copy(x_tab, bx, more.at[1]),
    ]
    tables[0].start()
    lax.fori_loop(0, blocks, begin, 0)
    tables[1].start()
    tables[0].wait()

    def one(b, carry):
        for c in copies(b):
            c.wait()
        first = pl.multiple_of(b * block, block)
        at = pl.ds(first, block)
        flag = bfl[at].astype(jnp.float32)
        fr = btr[at].astype(jnp.float32) * flag
        fi = bti[at].astype(jnp.float32) * flag
        for a in range(angles):
            br = bar[a, at].astype(jnp.float32)
            bi = bai[a, at].astype(jnp.float32)
            pr = (fr * br + fi * bi).astype(jnp.bfloat16).reshape(block * rows, size_z)
            pi = (fi * br - fr * bi).astype(jnp.bfloat16).reshape(block * rows, size_z)
            both = jnp.concatenate([pr, pi], 1)
            sums = jnp.dot(both, bz[...], preferred_element_type=jnp.float32)
            tmp[2 * a] = sums[:, :size_z]
            tmp[2 * a + 1] = sums[:, size_z:]
            for k in range(rows):
                half = [tmp[2 * a + h, pl.ds(k, block, stride=rows), :] for h in range(2)]
                q[a, k, at, :] = jnp.concatenate(half, 1).astype(jnp.bfloat16)
        return carry

    lax.fori_loop(0, blocks, one, 0)
    leaving = [pltpu.make_async_copy(q, q_out, more.at[2])]
    leaving[0].start()
    tables[1].wait()
    for a in range(angles):

        def put(value, a=a):
            sent[a] = value.reshape(sent.shape[1:])

        spin(q.at[a], bx, wide, put, 4)
        leaving.append(pltpu.make_async_copy(sent.at[a], sent_out.at[:, a], more.at[3 + a]))
        leaving[-1].start()
    for c in leaving:
        c.wait()


def along_x(q, table, out, tmp):
    def put(value):
        out[...] = value.reshape(out.shape)

    spin(q.at[0], table, tmp, put, 2)


def along_y(who, got, sigma, table, keep, send, *, scale):
    groups, angles, count, pair, size_z = got.shape
    me = who[0]
    part = table.shape[0] // 4
    starts = [pl.multiple_of(jnp.bitwise_xor(me, r) * part, part) for r in range(4)]
    left = jnp.concatenate([table[pl.ds(s, part), :] for s in starts], 0)
    sums = []
    for a in range(angles):
        right = jnp.concatenate([got[:, a, i].reshape(groups * pair, size_z) for i in range(count)], 1)
        sums.append(jnp.dot(left, right, preferred_element_type=jnp.float32))
    for i in range(count):
        for r in range(4):
            here = (slice(r * part, (r + 1) * part), slice(i * size_z, (i + 1) * size_z))
            inverse = scale / sigma[i, pl.ds(starts[r], part), :]
            best = sums[0][here] * inverse
            runner = jnp.full_like(best, -1e30)
            for a in range(1, angles):
                score = sums[a][here] * inverse
                runner = jnp.maximum(runner, jnp.minimum(best, score))
                best = jnp.maximum(best, score)
            to = send if r % 2 else keep
            to[r // 2, 0, i] = best.astype(jnp.bfloat16)
            to[r // 2, 1, i] = runner.astype(jnp.bfloat16)


def top_two(first, later):
    best = jnp.maximum(first[0], later[0])
    return best, jnp.maximum(jnp.minimum(first[0], later[0]), jnp.maximum(first[1], later[1]))


def join_core(mine, other, keep, send):
    for slot, to in enumerate((keep, send)):
        best, runner = top_two((mine[slot, 0], mine[slot, 1]), (other[slot, 0], other[slot, 1]))
        to[0] = best
        to[1] = runner


def join_far(mine, other, *outs):
    best, runner = top_two((mine[0], mine[1]), (other[0], other[1]))
    outs[-2][...] = best.astype(jnp.float32)
    outs[-1][...] = runner.astype(jnp.float32)


def cost(flops, moved):
    return pl.CostEstimate(flops=flops, bytes_accessed=moved, transcendentals=0)


def on_device(tomo_real, tomo_imag, template_real, template_imag, wedge_flags, local_sigma):
    size_x, rows, size_z = tomo_real.shape
    angles = template_real.shape[0]
    size_y = local_sigma.shape[1]
    groups = size_y // rows
    part = size_y // 4
    scale = 1.0 / math.sqrt(size_x * size_y * size_z)
    block = 64
    params = pltpu.CompilerParams(vmem_limit_bytes=48 * 1024 * 1024)

    anywhere = pl.BlockSpec(memory_space=pl.ANY)
    blocks = size_x // block
    vmem = pltpu.VMEM
    count = CHUNKS[0]
    table = x_table(size_x, groups, 0, count)
    whole = (size_x, rows, size_z)
    spectrum, piece = pl.pallas_call(
        front,
        in_specs=[anywhere] * 7,
        out_specs=[anywhere] * 2,
        out_shape=[
            jax.ShapeDtypeStruct((angles, rows, size_x, 2 * size_z), jnp.bfloat16),
            jax.ShapeDtypeStruct((groups, angles, count, 2 * rows, size_z), jnp.bfloat16),
        ],
        scratch_shapes=[
            vmem(whole, jnp.bfloat16),
            vmem(whole, jnp.bfloat16),
            vmem((angles,) + whole, jnp.bfloat16),
            vmem((angles,) + whole, jnp.bfloat16),
            vmem(whole, jnp.int32),
            vmem((2 * size_z, 2 * size_z), jnp.bfloat16),
            vmem(table.shape, jnp.bfloat16),
            vmem((2 * angles, block * rows, size_z), jnp.float32),
            vmem((angles, rows, size_x, 2 * size_z), jnp.bfloat16),
            vmem((2, groups * count * rows, size_z), jnp.float32),
            vmem((angles, groups, count, 2 * rows, size_z), jnp.bfloat16),
            pltpu.SemaphoreType.DMA((blocks, 5)),
            pltpu.SemaphoreType.DMA((3 + angles,)),
        ],
        compiler_params=pltpu.CompilerParams(vmem_limit_bytes=60 * 1024 * 1024),
        cost_estimate=cost(8 * angles * size_x * rows * size_z * size_z, 12 * 2**20),
        name="front",
    )(tomo_real, tomo_imag, template_real, template_imag, wedge_flags, z_table(size_z), table)

    me = lax.axis_index("angle").astype(jnp.int32)[None]
    columns = y_table(size_y, groups)
    first = 0
    results = ()
    for at, count in enumerate(CHUNKS):
        if at:
            table = x_table(size_x, groups, first, count)
            piece = pl.pallas_call(
                along_x,
                grid=(angles,),
                in_specs=[
                    pl.BlockSpec((1, rows, size_x, 2 * size_z), lambda a: (a, 0, 0, 0)),
                    pl.BlockSpec(table.shape, lambda a: (0, 0)),
                ],
                out_specs=pl.BlockSpec((groups, 1, count, 2 * rows, size_z), lambda a: (0, a, 0, 0, 0)),
                out_shape=jax.ShapeDtypeStruct((groups, angles, count, 2 * rows, size_z), jnp.bfloat16),
                scratch_shapes=[vmem((2, groups * count * rows, size_z), jnp.float32)],
                compiler_params=params,
                cost_estimate=cost(8 * angles * size_x * groups * count * rows * size_z, 8 * 2**20),
                name="along_x",
            )(spectrum, table)
        got = lax.all_to_all(piece, "pencil", split_axis=0, concat_axis=0, tiled=True)
        step = 2 if count % 2 == 0 and first % 2 == 0 else 1
        out = jax.ShapeDtypeStruct((2, 2, count, part, size_z), jnp.bfloat16)
        keep, send = pl.pallas_call(
            lambda *refs: along_y(*refs, scale=scale),
            grid=(count // step,),
            in_specs=[
                pl.BlockSpec(memory_space=pltpu.SMEM),
                pl.BlockSpec((groups, angles, step, 2 * rows, size_z), lambda i: (0, 0, i, 0, 0)),
                pl.BlockSpec((step, size_y, size_z), lambda i, o=first // step: (i + o, 0, 0)),
                pl.BlockSpec(columns.shape, lambda i: (0, 0)),
            ],
            out_specs=[pl.BlockSpec((2, 2, step, part, size_z), lambda i: (0, 0, i, 0, 0))] * 2,
            out_shape=[out, out],
            compiler_params=params,
            cost_estimate=cost(4 * angles * count * size_y * size_y * size_z, 2 * 2**20 * count),
            name="along_y",
        )(me, got, local_sigma, columns)
        other = lax.ppermute(send, "angle", CORE)
        near = jax.ShapeDtypeStruct((2, count, part, size_z), jnp.bfloat16)
        keep, send = pl.pallas_call(
            join_core,
            out_shape=[near, near],
            compiler_params=params,
            cost_estimate=cost(2**20 * count, 2**19 * count),
            name="join_core",
        )(keep, other)
        other = lax.ppermute(send, "angle", FAR)
        done = jax.ShapeDtypeStruct((local_sigma.shape[0], part, size_z), jnp.float32)
        narrow = pl.BlockSpec((2, step, part, size_z), lambda i: (0, i, 0, 0))
        results = pl.pallas_call(
            join_far,
            grid=(count // step,),
            in_specs=[narrow, narrow] + [anywhere] * len(results),
            out_specs=[pl.BlockSpec((step, part, size_z), lambda i, o=first // step: (i + o, 0, 0))] * 2,
            out_shape=[done, done],
            input_output_aliases={2: 0, 3: 1} if results else {},
            compiler_params=params,
            cost_estimate=cost(2**20, 2**21),
            name="join_far",
        )(keep, other, *results)
        first += count
    return tuple(results)


def solution(mesh):
    in_specs = (
        P(None, "pencil", None),
        P(None, "pencil", None),
        P("angle", None, "pencil", None),
        P("angle", None, "pencil", None),
        P(None, "pencil", None),
        P("pencil", None, None),
    )
    out_specs = (P("pencil", "angle", None), P("pencil", "angle", None))
    return jax.shard_map(on_device, mesh=mesh, in_specs=in_specs, out_specs=out_specs, check_vma=False)
```

```python
import math

import jax
import jax.numpy as jnp
import numpy as np
from jax import lax
from jax.experimental import pallas as pl
from jax.experimental.pallas import tpu as pltpu
from jax.sharding import PartitionSpec as P

CHUNKS = (6, 2)
CORE = ((0, 1), (1, 0), (2, 3), (3, 2))
FAR = ((0, 2), (1, 3), (2, 0), (3, 1))
SIDES = (4, 2, 8)
NEAR = tuple((dy, dx) for dy in range(SIDES[0]) for dx in range(SIDES[1]))


def place(at, dy, dx, dz):
    _, sx, sz = SIDES
    y = (at // (sx * sz) + dy) % SIDES[0]
    x = (at // sz + dx) % sx
    return (y * sx + x) * sz + (at + dz) % sz


def hop(dy, dx, dz):
    return tuple((p, place(p, dy, dx, dz)) for p in range(math.prod(SIDES)))


def phases(length):
    k = np.arange(length, dtype=np.int64)
    angle = (k[:, None] * k[None, :] % length) * (2.0 * math.pi / length)
    return np.cos(angle), np.sin(angle)


def z_table(size_z):
    cos, sin = phases(size_z)
    return np.concatenate([cos, sin], 1).astype(jnp.bfloat16)


def x_table(size_x, groups, first, count):
    cos, sin = phases(size_x)
    each = size_x // groups
    rows = (np.arange(groups)[:, None] * each + np.arange(first, first + count)[None, :]).reshape(-1)
    return np.concatenate([cos[rows], sin[rows]], 0).astype(jnp.bfloat16)


def y_table(size_y, groups):
    cos, sin = phases(size_y)
    both = np.stack([cos.reshape(size_y, groups, -1), -sin.reshape(size_y, groups, -1)], 2)
    return both.reshape(size_y, -1).astype(jnp.bfloat16)


def spin(q, table, tmp, unroll):
    rows, _, width = q.shape
    size_z = width // 2
    half = table.shape[0] // 2

    def one(k, carry):
        both = jnp.dot(table[...], q[k], preferred_element_type=jnp.float32)
        tmp[0, pl.ds(k, half, stride=rows), :] = both[:half, :size_z] - both[half:, size_z:]
        tmp[1, pl.ds(k, half, stride=rows), :] = both[half:, :size_z] + both[:half, size_z:]
        return carry

    lax.fori_loop(0, rows, one, 0, unroll=unroll)


def front(tr, ti, ar, ai, flags, z_tab, x_tab, q_out, sent_out, *scratch):
    btr, bti, bar, bai, bfl, bz, bx, tmp, q, wide, sent, sems, more = scratch
    angles, size_x, rows, size_z = bar.shape
    blocks = sems.shape[0]
    block = size_x // blocks

    def copies(b):
        at = pl.ds(pl.multiple_of(b * block, block), block)
        pairs = [(tr.at[at], btr.at[at]), (ti.at[at], bti.at[at]), (flags.at[at], bfl.at[at])]
        pairs += [(ar.at[:, at], bar.at[:, at]), (ai.at[:, at], bai.at[:, at])]
        return [pltpu.make_async_copy(s, d, sems.at[b, j]) for j, (s, d) in enumerate(pairs)]

    def begin(b, carry):
        for c in copies(b):
            c.start()
        return carry

    tables = [
        pltpu.make_async_copy(z_tab, bz.at[pl.ds(0, size_z)], more.at[0]),
        pltpu.make_async_copy(x_tab, bx, more.at[1]),
    ]
    tables[0].start()
    lax.fori_loop(0, blocks, begin, 0)
    tables[1].start()
    tables[0].wait()
    bz[size_z:, :size_z] = -bz[:size_z, size_z:]
    bz[size_z:, size_z:] = bz[:size_z, :size_z]

    def one(b, carry):
        for c in copies(b):
            c.wait()
        first = pl.multiple_of(b * block, block)
        at = pl.ds(first, block)
        flag = bfl[at].astype(jnp.float32)
        fr = btr[at].astype(jnp.float32) * flag
        fi = bti[at].astype(jnp.float32) * flag
        for a in range(angles):
            br = bar[a, at].astype(jnp.float32)
            bi = bai[a, at].astype(jnp.float32)
            pr = (fr * br + fi * bi).astype(jnp.bfloat16).reshape(block * rows, size_z)
            pi = (fi * br - fr * bi).astype(jnp.bfloat16).reshape(block * rows, size_z)
            both = jnp.concatenate([pr, pi], 1)
            sums = jnp.dot(both, bz[...], preferred_element_type=jnp.float32)
            tmp[2 * a] = sums[:, :size_z]
            tmp[2 * a + 1] = sums[:, size_z:]
            for k in range(rows):
                half = [tmp[2 * a + h, pl.ds(k, block, stride=rows), :] for h in range(2)]
                q[a, k, at, :] = jnp.concatenate(half, 1).astype(jnp.bfloat16)
        return carry

    lax.fori_loop(0, blocks, one, 0)
    leaving = [pltpu.make_async_copy(q, q_out, more.at[2])]
    leaving[0].start()
    tables[1].wait()
    for a in range(angles):
        spin(q.at[a], bx, wide, 2)
        pair = [wide[h].reshape(-1, rows, size_z) for h in range(2)]
        sent[a] = jnp.concatenate(pair, 1).astype(jnp.bfloat16).reshape(sent.shape[1:])
        leaving.append(pltpu.make_async_copy(sent.at[a], sent_out.at[:, a], more.at[3 + a]))
        leaving[-1].start()
    for c in leaving:
        c.wait()


def along_x(who, q, table, *rest):
    outs, tmp = rest[:-1], rest[-1]
    steps, _, count, pair, size_z = outs[0].shape
    rows = pair // 2
    each = count * rows
    spin(q.at[0], table, tmp, 1)
    for out, (dy, dx) in zip(outs, NEAR):
        for dz in range(steps):
            at = pl.ds(pl.multiple_of(place(who[0], dy, dx, dz) * each, each), each)
            halves = [tmp[h, at, :].reshape(count, rows, size_z) for h in range(2)]
            out[dz, 0] = jnp.concatenate(halves, 1).astype(jnp.bfloat16)


def regroup(*refs):
    half = len(refs) // 2
    for dz, out in enumerate(refs[half:]):
        for i, piece in enumerate(refs[:half]):
            out[i] = piece[dz]


def collect_along_y(who, me, *refs):
    pieces, (inverse, table, keep, send, got) = refs[:-5], refs[-5:]
    for dz, piece in enumerate(pieces):
        for i, (dy, dx) in enumerate(NEAR):
            got[place(me[0], SIDES[0] - dy, SIDES[1] - dx, SIDES[2] - dz)] = piece[i]
    along_y(who, got, inverse, table, keep, send)


def along_y(who, got, inverse, table, keep, send):
    groups, angles, count, pair, size_z = got.shape
    me = who[0]
    part = table.shape[0] // 4
    starts = [pl.multiple_of(jnp.bitwise_xor(me, r) * part, part) for r in range(4)]
    left = jnp.concatenate([table[pl.ds(s, part), :] for s in starts], 0)
    sums = []
    for a in range(angles):
        right = jnp.concatenate([got[:, a, i].reshape(groups * pair, size_z) for i in range(count)], 1)
        sums.append(jnp.dot(left, right, preferred_element_type=jnp.float32))
    for i in range(count):
        for r in range(4):
            here = (slice(r * part, (r + 1) * part), slice(i * size_z, (i + 1) * size_z))
            factor = inverse[i, pl.ds(starts[r], part), :]
            best = sums[0][here] * factor
            runner = jnp.full_like(best, -1e30)
            for a in range(1, angles):
                score = sums[a][here] * factor
                runner = jnp.maximum(runner, jnp.minimum(best, score))
                best = jnp.maximum(best, score)
            to = send if r % 2 else keep
            to[r // 2, 0, i] = best.astype(jnp.bfloat16)
            to[r // 2, 1, i] = runner.astype(jnp.bfloat16)


def invert(sigma, out, *, scale):
    out[...] = scale / sigma[...]


def top_two(first, later):
    best = jnp.maximum(first[0], later[0])
    return best, jnp.maximum(jnp.minimum(first[0], later[0]), jnp.maximum(first[1], later[1]))


def join_core(mine, other, keep, send):
    for slot, to in enumerate((keep, send)):
        best, runner = top_two((mine[slot, 0], mine[slot, 1]), (other[slot, 0], other[slot, 1]))
        to[0] = best
        to[1] = runner


def join_far(mine, other, *outs):
    best, runner = top_two((mine[0], mine[1]), (other[0], other[1]))
    outs[-2][...] = best.astype(jnp.float32)
    outs[-1][...] = runner.astype(jnp.float32)


def cost(flops, moved):
    return pl.CostEstimate(flops=flops, bytes_accessed=moved, transcendentals=0)


def on_device(tomo_real, tomo_imag, template_real, template_imag, wedge_flags, local_sigma):
    size_x, rows, size_z = tomo_real.shape
    angles = template_real.shape[0]
    size_y = local_sigma.shape[1]
    groups = size_y // rows
    part = size_y // 4
    scale = 1.0 / math.sqrt(size_x * size_y * size_z)
    block = 64
    params = pltpu.CompilerParams(vmem_limit_bytes=20 * 1024 * 1024)
    tight = pltpu.CompilerParams(vmem_limit_bytes=8 * 1024 * 1024)

    anywhere = pl.BlockSpec(memory_space=pl.ANY)
    blocks = size_x // block
    vmem = pltpu.VMEM
    count = CHUNKS[0]
    table = x_table(size_x, groups, 0, count)
    whole = (size_x, rows, size_z)
    spectrum, piece = pl.pallas_call(
        front,
        in_specs=[anywhere] * 7,
        out_specs=[anywhere] * 2,
        out_shape=[
            jax.ShapeDtypeStruct((angles, rows, size_x, 2 * size_z), jnp.bfloat16),
            jax.ShapeDtypeStruct((groups, angles, count, 2 * rows, size_z), jnp.bfloat16),
        ],
        scratch_shapes=[
            vmem(whole, jnp.bfloat16),
            vmem(whole, jnp.bfloat16),
            vmem((angles,) + whole, jnp.bfloat16),
            vmem((angles,) + whole, jnp.bfloat16),
            vmem(whole, jnp.int32),
            vmem((2 * size_z, 2 * size_z), jnp.bfloat16),
            vmem(table.shape, jnp.bfloat16),
            vmem((2 * angles, block * rows, size_z), jnp.float32),
            vmem((angles, rows, size_x, 2 * size_z), jnp.bfloat16),
            vmem((2, groups * count * rows, size_z), jnp.float32),
            vmem((angles, groups, count, 2 * rows, size_z), jnp.bfloat16),
            pltpu.SemaphoreType.DMA((blocks, 5)),
            pltpu.SemaphoreType.DMA((3 + angles,)),
        ],
        compiler_params=pltpu.CompilerParams(vmem_limit_bytes=60 * 1024 * 1024),
        cost_estimate=cost(8 * angles * size_x * rows * size_z * size_z, 12 * 2**20),
        name="front",
    )(tomo_real, tomo_imag, template_real, template_imag, wedge_flags, z_table(size_z), table)

    me = lax.axis_index("angle").astype(jnp.int32)[None]
    pencil = lax.axis_index("pencil").astype(jnp.int32)[None]
    columns = y_table(size_y, groups)
    scalar = pl.BlockSpec(memory_space=pltpu.SMEM)
    first, count = CHUNKS
    table = x_table(size_x, groups, first, count)
    steps = SIDES[2]
    bytes_out = 2 * groups * angles * count * 2 * rows * size_z

    def block_of(shape):
        return pl.BlockSpec(shape, lambda *_: (0,) * len(shape))

    got = lax.all_to_all(piece, "pencil", split_axis=0, concat_axis=0, tiled=True)
    pieces = pl.pallas_call(
        along_x,
        grid=(angles,),
        in_specs=[scalar, pl.BlockSpec((1, rows, size_x, 2 * size_z), lambda a: (a, 0, 0, 0)), block_of(table.shape)],
        out_specs=[pl.BlockSpec((steps, 1, count, 2 * rows, size_z), lambda a: (0, a, 0, 0, 0))]
        * len(NEAR),
        out_shape=[jax.ShapeDtypeStruct((steps, angles, count, 2 * rows, size_z), jnp.bfloat16)]
        * len(NEAR),
        scratch_shapes=[vmem((2, groups * count * rows, size_z), jnp.float32)],
        compiler_params=params,
        cost_estimate=cost(8 * angles * size_x * groups * count * rows * size_z, 8 * 2**20),
        name="along_x",
    )(pencil, spectrum, table)
    moved = [pieces[0]]
    for i in range(1, len(NEAR)):
        moved.append(lax.ppermute(pieces[i], "pencil", hop(*NEAR[i], 0)))
    pieces = pl.pallas_call(
        regroup,
        out_shape=[jax.ShapeDtypeStruct((len(NEAR), angles, count, 2 * rows, size_z), jnp.bfloat16)]
        * steps,
        compiler_params=tight,
        cost_estimate=cost(2**20, 2 * bytes_out),
        name="regroup",
    )(*moved)
    moved = [pieces[0]]
    for dz in range(1, steps):
        moved.append(lax.ppermute(pieces[dz], "pencil", hop(0, 0, dz)))
    inverse = pl.pallas_call(
        lambda *refs: invert(*refs, scale=scale),
        grid=(4,),
        in_specs=[pl.BlockSpec((local_sigma.shape[0] // 4, size_y, size_z), lambda i: (i, 0, 0))],
        out_specs=pl.BlockSpec((local_sigma.shape[0] // 4, size_y, size_z), lambda i: (i, 0, 0)),
        out_shape=jax.ShapeDtypeStruct(local_sigma.shape, jnp.float32),
        compiler_params=tight,
        cost_estimate=cost(2**20, 2**22),
        name="invert",
    )(local_sigma)

    def join(first, count, step, keep, send, results):
        other = lax.ppermute(send, "angle", CORE)
        near = jax.ShapeDtypeStruct((2, count, part, size_z), jnp.bfloat16)
        keep, send = pl.pallas_call(
            join_core,
            out_shape=[near, near],
            compiler_params=tight,
            cost_estimate=cost(2**20 * count, 2**19 * count),
            name="join_core",
        )(keep, other)
        other = lax.ppermute(send, "angle", FAR)
        done = jax.ShapeDtypeStruct((local_sigma.shape[0], part, size_z), jnp.float32)
        narrow = pl.BlockSpec((2, step, part, size_z), lambda i: (0, i, 0, 0))
        return pl.pallas_call(
            join_far,
            grid=(count // step,),
            in_specs=[narrow, narrow] + [anywhere] * len(results),
            out_specs=[pl.BlockSpec((step, part, size_z), lambda i: (i + first // step, 0, 0))] * 2,
            out_shape=[done, done],
            input_output_aliases={2: 0, 3: 1} if results else {},
            compiler_params=tight,
            cost_estimate=cost(2**20, 2**21),
            name="join_far",
        )(keep, other, *results)

    step = 2
    out_block = pl.BlockSpec((2, 2, step, part, size_z), lambda i: (0, 0, i, 0, 0))
    out = jax.ShapeDtypeStruct((2, 2, first, part, size_z), jnp.bfloat16)
    keep, send = pl.pallas_call(
        along_y,
        grid=(first // step,),
        in_specs=[
            scalar,
            pl.BlockSpec((groups, angles, step, 2 * rows, size_z), lambda i: (0, 0, i, 0, 0)),
            pl.BlockSpec((step, size_y, size_z), lambda i: (i, 0, 0)),
            block_of(columns.shape),
        ],
        out_specs=[out_block] * 2,
        out_shape=[out, out],
        compiler_params=params,
        cost_estimate=cost(4 * angles * first * size_y * size_y * size_z, 2 * 2**20 * first),
        name="along_y",
    )(me, got, inverse, columns)
    results = join(0, first, step, keep, send, ())
    out = jax.ShapeDtypeStruct((2, 2, count, part, size_z), jnp.bfloat16)
    keep, send = pl.pallas_call(
        collect_along_y,
        grid=(1,),
        in_specs=[scalar, scalar]
        + [block_of((len(NEAR), angles, count, 2 * rows, size_z))] * steps
        + [pl.BlockSpec((step, size_y, size_z), lambda i: (first // step, 0, 0)), block_of(columns.shape)],
        out_specs=[out_block] * 2,
        out_shape=[out, out],
        scratch_shapes=[vmem((groups, angles, count, 2 * rows, size_z), jnp.bfloat16)],
        compiler_params=params,
        cost_estimate=cost(4 * angles * count * size_y * size_y * size_z, 2 * 2**20 * count),
        name="along_y",
    )(me, pencil, *moved, inverse, columns)
    return tuple(join(first, count, step, keep, send, results))


def solution(mesh):
    in_specs = (
        P(None, "pencil", None),
        P(None, "pencil", None),
        P("angle", None, "pencil", None),
        P("angle", None, "pencil", None),
        P(None, "pencil", None),
        P("pencil", None, None),
    )
    out_specs = (P("pencil", "angle", None), P("pencil", "angle", None))
    return jax.shard_map(on_device, mesh=mesh, in_specs=in_specs, out_specs=out_specs, check_vma=False)
```
